16 devices in a mesh: dp: 2 (over z), cp: 8 (over y, x, core).
Axes of the slice: x: 2, y: 2, z: 2, core: 2. Of those that a mesh axis runs over, the one named last changes fastest.
Arguments:
- x_in: bfloat16 [16, 512, 2048], P('dp', 'cp'), parts along dimension 0
- positions: int32 [1024], P(('dp', 'cp')), parts along dimension 0
- long_factor: float32 [32], replicated
- norm_gain: float32 [2048], replicated
- w_qkv: bfloat16 [2048, 6144], replicated
- w_out: bfloat16 [2048, 2048], replicated
- grad_y: bfloat16 [16, 512, 2048], P('dp', 'cp'), parts along dimension 0
Outputs:
- output 1: bfloat16 [16, 512, 2048], P('dp', 'cp'), parts along dimension 0
- output 2: bfloat16 [16, 512, 2048], P('dp', 'cp'), parts along dimension 0
- output 3: float32 [4096], P('dp'), parts along dimension 0
- output 4: float32 [4096, 6144], P('dp'), parts along dimension 0
- output 5: float32 [4096, 2048], P('dp'), parts along dimension 0
There are 2 independent parts. The reference program is written for one: setup_inputs(seed, part) draws one part's arguments, and reference() takes and returns one part's arrays. A program takes and returns all parts, laid end to end along the dimension named above; an argument that names none is the same for every part.
All inputs are finite; a program needn't handle non-finite values.
Results may differ from the reference program's by a relative error of at most 0.014743.
Values are sent between devices in bfloat16 or wider.
A program may use at most 1 GiB of HBM per device.

```python
import math
import jax
import jax.numpy as jnp
from jax import lax

BATCH = 8
SEQ_LEN = 512
HIDDEN = 2048
HEADS = 32
HEAD_DIM = 64
HALF_DIM = HEAD_DIM // 2
WIDTH = HEADS * HEAD_DIM
NORM_EPS = 1e-5
MSCALE = math.sqrt(1.0 + math.log(32.0) / math.log(4096.0))
SCALE = 1.0 / math.sqrt(HEAD_DIM)
QK_GAIN = 1.6
MASK_VALUE = -1e30


def setup_inputs(seed: int = 0, part: int = 0) -> dict:
    part_keys = jax.random.split(jax.random.fold_in(jax.random.key(seed), part), 3)
    shared_keys = jax.random.split(jax.random.key(seed + 1), 4)
    x_in = jax.random.normal(part_keys[0], (BATCH, SEQ_LEN, HIDDEN), jnp.float32)
    gaps = jax.random.randint(part_keys[1], (SEQ_LEN,), 1, 3)
    positions = (jnp.cumsum(gaps) - 1).astype(jnp.int32)
    grad_y = jax.random.normal(part_keys[2], (BATCH, SEQ_LEN, HIDDEN), jnp.float32)
    long_factor = jnp.exp(jax.random.uniform(shared_keys[0], (HALF_DIM,), jnp.float32, 0.0, 2.5))
    norm_gain = jax.random.uniform(shared_keys[1], (HIDDEN,), jnp.float32, 0.5, 1.5)
    col_gain = jnp.concatenate([jnp.full((2 * WIDTH,), QK_GAIN, jnp.float32), jnp.ones((WIDTH,), jnp.float32)])
    w_qkv = jax.random.normal(shared_keys[2], (HIDDEN, 3 * WIDTH), jnp.float32) * (HIDDEN ** -0.5) * col_gain
    w_out = jax.random.normal(shared_keys[3], (WIDTH, HIDDEN), jnp.float32) * (WIDTH ** -0.5)
    return {'x_in': x_in.astype(jnp.bfloat16), 'positions': positions, 'long_factor': long_factor, 'norm_gain': norm_gain, 'w_qkv': w_qkv.astype(jnp.bfloat16), 'w_out': w_out.astype(jnp.bfloat16), 'grad_y': grad_y.astype(jnp.bfloat16)}


def rope_tables(positions, long_factor):
    exponent = jnp.arange(HALF_DIM, dtype=jnp.float32) * (2.0 / HEAD_DIM)
    inv_freq = 1.0 / (long_factor * jnp.power(10000.0, exponent))
    angles = positions.astype(jnp.float32)[:, None] * inv_freq[None, :]
    angle_pair = jnp.concatenate([angles, angles], axis=-1)
    return jnp.cos(angle_pair) * MSCALE, jnp.sin(angle_pair) * MSCALE


def rotate_half(values):
    return jnp.concatenate([-values[..., HALF_DIM:], values[..., :HALF_DIM]], axis=-1)


def head_attention(blocks):
    q_head, k_head, v_head = blocks
    scores = jnp.einsum('bqd,bkd->bqk', q_head.astype(jnp.float32), k_head.astype(jnp.float32)) * SCALE
    token_idx = jnp.arange(SEQ_LEN)
    scores = jnp.where(token_idx[None, :, None] >= token_idx[None, None, :], scores, MASK_VALUE)
    attn_probs = jax.nn.softmax(scores, axis=-1).astype(jnp.bfloat16)
    return jnp.einsum('bqk,bkd->bqd', attn_probs.astype(jnp.float32), v_head.astype(jnp.float32)).astype(jnp.bfloat16)


def heads_first(tensor):
    return jnp.transpose(tensor, (2, 0, 1, 3))


def block_forward(x_in, norm_gain, w_qkv32, w_out32, cos_tab, sin_tab):
    x_float = x_in.astype(jnp.float32)
    inv_rms = lax.rsqrt(jnp.mean(x_float * x_float, axis=-1, keepdims=True) + NORM_EPS)
    normed = (x_float * inv_rms * norm_gain).astype(jnp.bfloat16)
    qkv_all = jnp.dot(normed.reshape(BATCH * SEQ_LEN, HIDDEN).astype(jnp.float32), w_qkv32)
    qkv_all = qkv_all.reshape(BATCH, SEQ_LEN, 3, HEADS, HEAD_DIM)
    cos_b = cos_tab[None, :, None, :]
    sin_b = sin_tab[None, :, None, :]
    q_rot = (qkv_all[:, :, 0] * cos_b + rotate_half(qkv_all[:, :, 0]) * sin_b).astype(jnp.bfloat16)
    k_rot = (qkv_all[:, :, 1] * cos_b + rotate_half(qkv_all[:, :, 1]) * sin_b).astype(jnp.bfloat16)
    v_val = qkv_all[:, :, 2].astype(jnp.bfloat16)
    attn_out = lax.map(jax.checkpoint(head_attention), (heads_first(q_rot), heads_first(k_rot), heads_first(v_val)))
    attn_flat = jnp.transpose(attn_out, (1, 2, 0, 3)).reshape(BATCH * SEQ_LEN, WIDTH)
    proj = jnp.dot(attn_flat.astype(jnp.float32), w_out32).reshape(BATCH, SEQ_LEN, HIDDEN)
    return (x_float + proj).astype(jnp.bfloat16)


def reference(x_in, positions, long_factor, norm_gain, w_qkv, w_out, grad_y):
    cos_tab, sin_tab = rope_tables(positions, long_factor)

    def run(x_val, gain, w_first, w_second):
        return block_forward(x_val, gain, w_first, w_second, cos_tab, sin_tab)

    y_out, pullback = jax.vjp(run, x_in, norm_gain, w_qkv.astype(jnp.float32), w_out.astype(jnp.float32))
    grad_x, grad_gain, grad_wqkv, grad_wout = pullback(grad_y)
    return y_out, grad_x, grad_gain, grad_wqkv, grad_wout
```

```python
import functools
import math
import jax
import jax.numpy as jnp
from jax import lax
from jax.experimental import pallas as pl
from jax.experimental.pallas import tpu as pltpu
from jax.sharding import PartitionSpec as P

NORM_EPS = 1e-5
MSCALE = math.sqrt(1.0 + math.log(32.0) / math.log(4096.0))
MASK_VALUE = -1e30
F32 = jnp.float32
BF16 = jnp.bfloat16


def rope_tables(positions, long_factor):
    half = long_factor.shape[0]
    exponent = jnp.arange(half, dtype=F32) * (1.0 / half)
    inv_freq = 1.0 / (long_factor * jnp.power(10000.0, exponent))
    angles = positions.astype(F32)[:, None] * inv_freq[None, :]
    cos, sin = jnp.cos(angles) * MSCALE, jnp.sin(angles) * MSCALE
    return jnp.concatenate([cos] * 4, axis=1), jnp.concatenate([-sin, sin, -sin, sin], axis=1)


def dot(a, b, dims=((1,), (0,))):
    return lax.dot_general(a, b, (dims, ((), ())), preferred_element_type=F32)


def partner(t, first_half):
    width = t.shape[-1]
    return jnp.where(first_half, pltpu.roll(t, width - 32, 1), pltpu.roll(t, 32, 1))


def block_kernel(scale, x_ref, r_ref, dy_ref, gain_ref, wq_ref, wk_ref, wv_ref, wo_ref, cos_ref, sin_ref,
                 y_ref, dx_ref, gg_ref, ot_ref, dq_ref, dk_ref, dv_ref, y_acc, dn_acc):
    step = pl.program_id(0)
    seq = x_ref.shape[0]
    qb = 256

    @pl.when(step == 0)
    def _():
        y_acc[...] = x_ref[...].astype(F32)
        dn_acc[...] = jnp.zeros_like(dn_acc)

    r = r_ref[...]
    q_all = dot(r, wq_ref[...])
    k_all = dot(r, wk_ref[...])
    v_all = dot(r, wv_ref[...]).astype(BF16)
    da_all = dot(dy_ref[...], wo_ref[...], ((1,), (1,))).astype(BF16)
    cos, sin = cos_ref[...], sin_ref[...]
    lane = lax.broadcasted_iota(jnp.int32, (seq, 128), 1)
    first_half = (lane % 64) < 32
    head0 = lane < 64
    tri = lax.broadcasted_iota(jnp.int32, (qb, qb), 0) <= lax.broadcasted_iota(jnp.int32, (qb, qb), 1)
    zero_rows = jnp.zeros((64, seq), BF16)
    zero_pair = jnp.zeros((seq, 128), BF16)

    for pair in range(2):
        cols = slice(128 * pair, 128 * pair + 128)
        qf, kf = q_all[:, cols], k_all[:, cols]
        q = ((qf * cos + partner(qf, first_half) * sin).astype(BF16) * scale).astype(BF16)
        k = (kf * cos + partner(kf, first_half) * sin).astype(BF16)
        v, da = v_all[:, cols], da_all[:, cols]
        qt, kt, vt, dat = q.T, k.T, v.T, da.T
        ots, dqts = [], []
        dk_sum = [jnp.zeros((qb, 128), F32), jnp.zeros((qb, 128), F32)]
        dv_sum = [jnp.zeros((qb, 128), F32), jnp.zeros((qb, 128), F32)]
        for head in range(2):
            rows = slice(64 * head, 64 * head + 64)
            if head == 0:
                qt_h = jnp.concatenate([qt[rows], zero_rows], axis=0)
                dat_h = jnp.concatenate([dat[rows], zero_rows], axis=0)
                q_h = jnp.where(head0, q, zero_pair)
                da_h = jnp.where(head0, da, zero_pair)
            else:
                qt_h = jnp.concatenate([zero_rows, qt[rows]], axis=0)
                dat_h = jnp.concatenate([zero_rows, dat[rows]], axis=0)
                q_h = jnp.where(head0, zero_pair, q)
                da_h = jnp.where(head0, zero_pair, da)
            kt_h, vt_h = kt[rows], vt[rows]
            ot_b, dqt_b = [], []
            for blk in range(2):
                qs = slice(qb * blk, qb * blk + qb)
                nk = qb * (blk + 1)
                st = dot(k[:nk], qt_h[:, qs])
                if blk == 0:
                    st = jnp.where(tri, st, MASK_VALUE)
                else:
                    st = jnp.concatenate([st[:qb], jnp.where(tri, st[qb:], MASK_VALUE)], axis=0)
                m = jnp.max(st, axis=0, keepdims=True)
                e = jnp.exp(st - m)
                p = e * (1.0 / jnp.sum(e, axis=0, keepdims=True))
                pb = p.astype(BF16)
                ot = dot(vt_h[:, :nk], pb)
                ob = ot.astype(BF16)
                delta = jnp.sum(dat[rows, qs].astype(F32) * ob.astype(F32), axis=0, keepdims=True)
                dpt = dot(v[:nk], dat_h[:, qs])
                dsb = (p * (dpt - delta)).astype(BF16)
                dqt_b.append(dot(kt_h[:, :nk], dsb))
                ot_b.append(ob)
                dv_part = dot(pb, da_h[qs])
                dk_part = dot(dsb, q_h[qs])
                for half in range(blk + 1):
                    hs = slice(qb * half, qb * half + qb)
                    dv_sum[half] += dv_part[hs]
                    dk_sum[half] += dk_part[hs]
            ots.append(jnp.concatenate(ot_b, axis=1))
            dqts.append(jnp.concatenate(dqt_b, axis=1))
        ot_pair = jnp.concatenate(ots, axis=0)
        ot_ref[cols, :] = ot_pair
        o = ot_pair.T
        dq = jnp.concatenate(dqts, axis=0).T * scale
        dk = jnp.concatenate(dk_sum, axis=0)
        dv = jnp.concatenate(dv_sum, axis=0)
        dqb = (dq * cos - partner(dq, first_half) * sin).astype(BF16)
        dkb = (dk * cos - partner(dk, first_half) * sin).astype(BF16)
        dvb = dv.astype(BF16)
        dq_ref[:, cols] = dqb
        dk_ref[:, cols] = dkb
        dv_ref[:, cols] = dvb
        y_acc[...] += dot(o, wo_ref[cols, :])

    dn_acc[...] += (dot(dq_ref[...], wq_ref[...], ((1,), (1,))) + dot(dk_ref[...], wk_ref[...], ((1,), (1,)))
                    + dot(dv_ref[...], wv_ref[...], ((1,), (1,))))

    @pl.when(step == pl.num_programs(0) - 1)
    def _():
        y_ref[...] = y_acc[...].astype(BF16)
        x = x_ref[...].astype(F32)
        inv = lax.rsqrt(jnp.mean(x * x, axis=1, keepdims=True) + NORM_EPS)
        x_hat = x * inv
        dn = dn_acc[...]
        gg_ref[...] = jnp.sum(dn * x_hat, axis=0, keepdims=True)
        d_hat = dn * gain_ref[...]
        dx = inv * (d_hat - x_hat * jnp.mean(d_hat * x_hat, axis=1, keepdims=True))
        dx_ref[...] = (dy_ref[...].astype(F32) + dx).astype(BF16)


def block_call(x, r, dy, gain, w_qkv, w_out, cos, sin, scale):
    seq, hidden = x.shape
    width = w_out.shape[0]
    hb = 256
    steps = width // hb
    whole = lambda a: pl.BlockSpec(a.shape, lambda j: (0, 0), pipeline_mode=pl.Buffered(1))
    wcol = lambda part: pl.BlockSpec((hidden, hb), lambda j, part=part: (0, part * steps + j))
    tok = pl.BlockSpec((seq, hb), lambda j: (0, j))
    full = lambda s: pl.BlockSpec(s, lambda j: (0, 0))
    return pl.pallas_call(
        functools.partial(block_kernel, scale),
        grid=(steps,),
        in_specs=[whole(x), whole(r), whole(dy), whole(gain), wcol(0), wcol(1), wcol(2),
                  pl.BlockSpec((hb, hidden), lambda j: (j, 0)), whole(cos), whole(sin)],
        out_specs=[full((seq, hidden)), full((seq, hidden)), full((1, hidden)), pl.BlockSpec((hb, seq), lambda j: (j, 0)), tok, tok, tok],
        out_shape=[jax.ShapeDtypeStruct((seq, hidden), BF16), jax.ShapeDtypeStruct((seq, hidden), BF16),
                   jax.ShapeDtypeStruct((1, hidden), F32), jax.ShapeDtypeStruct((width, seq), BF16)]
        + [jax.ShapeDtypeStruct((seq, width), BF16)] * 3,
        scratch_shapes=[pltpu.VMEM((seq, hidden), F32), pltpu.VMEM((seq, hidden), F32)],
        compiler_params=pltpu.CompilerParams(dimension_semantics=("arbitrary",), vmem_limit_bytes=60 << 20),
        cost_estimate=pl.CostEstimate(flops=60_000_000_000, bytes_accessed=60_000_000, transcendentals=8_000_000),
        name="block",
    )(x, r, dy, gain, w_qkv, w_qkv, w_qkv, w_out, cos, sin)


def norm_kernel(x_ref, dy_ref, gain_ref, r_ref, pair_ref):
    x = x_ref[...].astype(F32)
    inv = lax.rsqrt(jnp.mean(x * x, axis=1, keepdims=True) + NORM_EPS)
    r = (x * inv * gain_ref[...]).astype(BF16)
    r_ref[...] = r
    pair_ref[0] = r.T
    pair_ref[1] = dy_ref[...].T


def norm_call(x, dy, gain):
    seq, hidden = x.shape
    return pl.pallas_call(
        norm_kernel,
        out_shape=[jax.ShapeDtypeStruct((seq, hidden), BF16), jax.ShapeDtypeStruct((2, hidden, seq), BF16)],
        compiler_params=pltpu.CompilerParams(vmem_limit_bytes=40 << 20),
        cost_estimate=pl.CostEstimate(flops=10_000_000, bytes_accessed=10_000_000, transcendentals=0),
        name="norm",
    )(x, dy, gain)


def grad_kernel(flip, a_ref, b_ref, *rest):
    out_ref = rest[-1]
    dims = ((1,), (1,)) if flip else ((1,), (0,))
    part = dot(a_ref[0, 0], b_ref[0, 0], dims)
    for i in range(1, a_ref.shape[0]):
        part += dot(a_ref[i, 0], b_ref[i, 0], dims)

    @pl.when(pl.program_id(2) == 0)
    def _():
        out_ref[...] = part

    @pl.when(pl.program_id(2) > 0)
    def _():
        out_ref[...] += part


def grad_call(at, b, n_out, col, buf=None, flip=False):
    n_seq, _, rows, seq = at.shape
    last = b.shape[1] - 1
    n = b.shape[2] if flip else b.shape[3]
    tm, tn, ts = 1024, 512, 2
    specs = [pl.BlockSpec((ts, 1, tm, seq), lambda i, j, k: (k, 0, i, 0)),
             pl.BlockSpec((ts, 1, tn, seq), lambda i, j, k: (k, last, j, 0)) if flip else pl.BlockSpec((ts, 1, seq, tn), lambda i, j, k: (k, last, 0, j))]
    args = [at, b]
    aliases = {}
    if buf is not None:
        specs.append(pl.BlockSpec(memory_space=pl.ANY))
        args.append(buf)
        aliases = {2: 0}
    return pl.pallas_call(
        functools.partial(grad_kernel, flip),
        grid=(rows // tm, n // tn, n_seq // ts),
        in_specs=specs,
        out_specs=pl.BlockSpec((tm, tn), lambda i, j, k: (i, col // tn + j)),
        out_shape=jax.ShapeDtypeStruct((rows, n_out), F32),
        input_output_aliases=aliases,
        compiler_params=pltpu.CompilerParams(dimension_semantics=("arbitrary",) * 3, vmem_limit_bytes=48 << 20),
        cost_estimate=pl.CostEstimate(flops=2 * rows * n * n_seq * seq, bytes_accessed=80_000_000, transcendentals=0),
        name="wgrad",
    )(*args)


def solution(mesh):
    def device_fn(x_in, positions, long_factor, norm_gain, w_qkv, w_out, grad_y):
        _, piece, hidden = x_in.shape
        n_dev = mesh.shape['cp']
        seq = piece * n_dev
        width = w_out.shape[0]
        scale = 1.0 / math.sqrt(2 * long_factor.shape[0])
        swap = lambda t: lax.all_to_all(t, 'cp', split_axis=0, concat_axis=0)
        x = swap(x_in).reshape(seq, hidden)
        dy = swap(grad_y).reshape(seq, hidden)
        pos = lax.all_gather(positions, 'cp', tiled=True)
        cos, sin = rope_tables(pos, long_factor)
        r, pair = norm_call(x, dy, norm_gain[None, :])
        gather = lambda t: lax.all_gather(t[None] if t.ndim == 2 else t, 'cp')
        pair_all = gather(pair)
        y, dx, gg, ot, dq, dk, dv = block_call(x, r, dy, norm_gain[None, :], w_qkv, w_out, cos, sin, scale)
        ot_all, dq_all, dk_all, dv_all = gather(ot), gather(dq), gather(dk), gather(dv)
        y_out = swap(y.reshape(n_dev, piece, hidden))
        grad_x = swap(dx.reshape(n_dev, piece, hidden))
        g_gain = lax.psum(gg[0], 'cp')
        g_wout = grad_call(ot_all, pair_all, hidden, 0, flip=True)
        g_wqkv = grad_call(pair_all, dq_all, 3 * width, 0)
        g_wqkv = grad_call(pair_all, dk_all, 3 * width, width, g_wqkv)
        g_wqkv = grad_call(pair_all, dv_all, 3 * width, 2 * width, g_wqkv)
        return y_out, grad_x, g_gain, g_wqkv, g_wout

    seq_spec = P('dp', 'cp', None)
    return jax.shard_map(device_fn, mesh=mesh, in_specs=(seq_spec, P(('dp', 'cp')), P(None), P(None), P(None, None), P(None, None), seq_spec), out_specs=(seq_spec, seq_spec, P('dp'), P('dp', None), P('dp', None)), check_vma=False)
```

```python
import functools
import math
import jax
import jax.numpy as jnp
from jax import lax
from jax.experimental import pallas as pl
from jax.experimental.pallas import tpu as pltpu
from jax.sharding import PartitionSpec as P

NORM_EPS = 1e-5
MSCALE = math.sqrt(1.0 + math.log(32.0) / math.log(4096.0))
MASK_VALUE = -1e30
F32 = jnp.float32
BF16 = jnp.bfloat16


def rope_tables(positions, long_factor):
    half = long_factor.shape[0]
    exponent = jnp.arange(half, dtype=F32) * (1.0 / half)
    inv_freq = 1.0 / (long_factor * jnp.power(10000.0, exponent))
    angles = positions.astype(F32)[:, None] * inv_freq[None, :]
    cos, sin = jnp.cos(angles) * MSCALE, jnp.sin(angles) * MSCALE
    return jnp.concatenate([cos] * 4, axis=1), jnp.concatenate([-sin, sin, -sin, sin], axis=1)


def dot(a, b, dims=((1,), (0,))):
    return lax.dot_general(a, b, (dims, ((), ())), preferred_element_type=F32)


def partner(t, first_half):
    width = t.shape[-1]
    return jnp.where(first_half, pltpu.roll(t, width - 32, 1), pltpu.roll(t, 32, 1))


def block_kernel(scale, x_ref, r_ref, dy_ref, gain_ref, wq_ref, wk_ref, wv_ref, wo_ref, cos_ref, sin_ref,
                 y_ref, dx_ref, gg_ref, oa_ref, ob_ref, qa_ref, qb_ref, ka_ref, kb_ref, va_ref, vb_ref, y_acc, dn_acc):
    step = pl.program_id(0)
    seq = x_ref.shape[0]
    qb = 256

    @pl.when(step == 0)
    def _():
        y_acc[...] = x_ref[...].astype(F32)
        dn_acc[...] = jnp.zeros_like(dn_acc)

    r = r_ref[...]
    q_all = dot(r, wq_ref[...])
    k_all = dot(r, wk_ref[...])
    v_all = dot(r, wv_ref[...]).astype(BF16)
    da_all = dot(dy_ref[...], wo_ref[...], ((1,), (1,))).astype(BF16)
    cos, sin = cos_ref[...], sin_ref[...]
    lane = lax.broadcasted_iota(jnp.int32, (seq, 128), 1)
    first_half = (lane % 64) < 32
    head0 = lane < 64
    tri = lax.broadcasted_iota(jnp.int32, (qb, qb), 0) <= lax.broadcasted_iota(jnp.int32, (qb, qb), 1)
    zero_rows = jnp.zeros((64, seq), BF16)
    zero_pair = jnp.zeros((seq, 128), BF16)

    for pair in range(2):
        cols = slice(128 * pair, 128 * pair + 128)
        qf, kf = q_all[:, cols], k_all[:, cols]
        q = ((qf * cos + partner(qf, first_half) * sin).astype(BF16) * scale).astype(BF16)
        k = (kf * cos + partner(kf, first_half) * sin).astype(BF16)
        v, da = v_all[:, cols], da_all[:, cols]
        qt, kt, vt, dat = q.T, k.T, v.T, da.T
        ots, dqts = [], []
        dk_sum = [jnp.zeros((qb, 128), F32), jnp.zeros((qb, 128), F32)]
        dv_sum = [jnp.zeros((qb, 128), F32), jnp.zeros((qb, 128), F32)]
        for head in range(2):
            rows = slice(64 * head, 64 * head + 64)
            if head == 0:
                qt_h = jnp.concatenate([qt[rows], zero_rows], axis=0)
                dat_h = jnp.concatenate([dat[rows], zero_rows], axis=0)
                q_h = jnp.where(head0, q, zero_pair)
                da_h = jnp.where(head0, da, zero_pair)
            else:
                qt_h = jnp.concatenate([zero_rows, qt[rows]], axis=0)
                dat_h = jnp.concatenate([zero_rows, dat[rows]], axis=0)
                q_h = jnp.where(head0, zero_pair, q)
                da_h = jnp.where(head0, zero_pair, da)
            kt_h, vt_h = kt[rows], vt[rows]
            ot_b, dqt_b = [], []
            for blk in range(2):
                qs = slice(qb * blk, qb * blk + qb)
                nk = qb * (blk + 1)
                st = dot(k[:nk], qt_h[:, qs])
                if blk == 0:
                    st = jnp.where(tri, st, MASK_VALUE)
                else:
                    st = jnp.concatenate([st[:qb], jnp.where(tri, st[qb:], MASK_VALUE)], axis=0)
                m = jnp.max(st, axis=0, keepdims=True)
                e = jnp.exp(st - m)
                p = e * (1.0 / jnp.sum(e, axis=0, keepdims=True))
                pb = p.astype(BF16)
                ot = dot(vt_h[:, :nk], pb)
                ob = ot.astype(BF16)
                delta = jnp.sum(dat[rows, qs].astype(F32) * ob.astype(F32), axis=0, keepdims=True)
                dpt = dot(v[:nk], dat_h[:, qs])
                dsb = (p * (dpt - delta)).astype(BF16)
                dqt_b.append(dot(kt_h[:, :nk], dsb))
                ot_b.append(ob)
                dv_part = dot(pb, da_h[qs])
                dk_part = dot(dsb, q_h[qs])
                for half in range(blk + 1):
                    hs = slice(qb * half, qb * half + qb)
                    dv_sum[half] += dv_part[hs]
                    dk_sum[half] += dk_part[hs]
            ots.append(jnp.concatenate(ot_b, axis=1))
            dqts.append(jnp.concatenate(dqt_b, axis=1))
        ot_pair = jnp.concatenate(ots, axis=0)
        o = ot_pair.T
        dq = jnp.concatenate(dqts, axis=0).T * scale
        dk = jnp.concatenate(dk_sum, axis=0)
        dv = jnp.concatenate(dv_sum, axis=0)
        dqb = (dq * cos - partner(dq, first_half) * sin).astype(BF16)
        dkb = (dk * cos - partner(dk, first_half) * sin).astype(BF16)
        dvb = dv.astype(BF16)
        for value, a_ref, b_ref in ((o, oa_ref, ob_ref), (dqb, qa_ref, qb_ref), (dkb, ka_ref, kb_ref), (dvb, va_ref, vb_ref)):
            a_ref[:, cols] = value[:qb]
            b_ref[:, cols] = value[qb:]
        y_acc[...] += dot(o, wo_ref[cols, :])

    for rows, dq_ref, dk_ref, dv_ref in ((slice(0, qb), qa_ref, ka_ref, va_ref), (slice(qb, 2 * qb), qb_ref, kb_ref, vb_ref)):
        dn_acc[rows, :] += (dot(dq_ref[...], wq_ref[...], ((1,), (1,))) + dot(dk_ref[...], wk_ref[...], ((1,), (1,)))
                            + dot(dv_ref[...], wv_ref[...], ((1,), (1,))))

    @pl.when(step == pl.num_programs(0) - 1)
    def _():
        y_ref[...] = y_acc[...].astype(BF16)
        x = x_ref[...].astype(F32)
        inv = lax.rsqrt(jnp.mean(x * x, axis=1, keepdims=True) + NORM_EPS)
        x_hat = x * inv
        dn = dn_acc[...]
        gg_ref[...] = jnp.sum(dn * x_hat, axis=0, keepdims=True)
        d_hat = dn * gain_ref[...]
        dx = inv * (d_hat - x_hat * jnp.mean(d_hat * x_hat, axis=1, keepdims=True))
        dx_ref[...] = (dy_ref[...].astype(F32) + dx).astype(BF16)


def block_call(x, r, dy, gain, w_qkv, w_out, cos, sin, scale):
    seq, hidden = x.shape
    width = w_out.shape[0]
    hb = 256
    steps = width // hb
    whole = lambda a: pl.BlockSpec(a.shape, lambda j: (0, 0), pipeline_mode=pl.Buffered(1))
    wcol = lambda part: pl.BlockSpec((hidden, hb), lambda j, part=part: (0, part * steps + j))
    tok = pl.BlockSpec((seq // 2, hb), lambda j: (0, j))
    full = lambda s: pl.BlockSpec(s, lambda j: (0, 0))
    return pl.pallas_call(
        functools.partial(block_kernel, scale),
        grid=(steps,),
        in_specs=[whole(x), whole(r), whole(dy), whole(gain), wcol(0), wcol(1), wcol(2),
                  pl.BlockSpec((hb, hidden), lambda j: (j, 0)), whole(cos), whole(sin)],
        out_specs=[full((seq, hidden)), full((seq, hidden)), full((1, hidden))] + [tok] * 8,
        out_shape=[jax.ShapeDtypeStruct((seq, hidden), BF16), jax.ShapeDtypeStruct((seq, hidden), BF16),
                   jax.ShapeDtypeStruct((1, hidden), F32)] + [jax.ShapeDtypeStruct((seq // 2, width), BF16)] * 8,
        scratch_shapes=[pltpu.VMEM((seq, hidden), F32), pltpu.VMEM((seq, hidden), F32)],
        compiler_params=pltpu.CompilerParams(dimension_semantics=("arbitrary",), vmem_limit_bytes=60 << 20),
        cost_estimate=pl.CostEstimate(flops=60_000_000_000, bytes_accessed=60_000_000, transcendentals=8_000_000),
        name="block",
    )(x, r, dy, gain, w_qkv, w_qkv, w_qkv, w_out, cos, sin)


def norm_kernel(x_ref, dy_ref, gain_ref, r_ref, *pair_refs):
    x = x_ref[...].astype(F32)
    inv = lax.rsqrt(jnp.mean(x * x, axis=1, keepdims=True) + NORM_EPS)
    r = (x * inv * gain_ref[...]).astype(BF16)
    r_ref[...] = r
    part = pair_refs[0].shape[2]
    for i, ref in enumerate(pair_refs):
        ref[0] = r[part * i:part * i + part].T
        ref[1] = dy_ref[part * i:part * i + part, :].T


def norm_call(x, dy, gain):
    seq, hidden = x.shape
    return pl.pallas_call(
        norm_kernel,
        out_shape=[jax.ShapeDtypeStruct((seq, hidden), BF16)] + [jax.ShapeDtypeStruct((2, hidden, seq // 2), BF16)] * 2,
        compiler_params=pltpu.CompilerParams(vmem_limit_bytes=40 << 20),
        cost_estimate=pl.CostEstimate(flops=10_000_000, bytes_accessed=10_000_000, transcendentals=0),
        name="norm",
    )(x, dy, gain)


def grad_kernel(count, flip, add, *refs):
    lefts, rights = refs[:count], refs[count:2 * count]
    out_ref, l_buf, r_buf = refs[-3:]
    part = lefts[0].shape[2]

    @pl.when(pl.program_id(1) == 0)
    def _():
        for i, ref in enumerate(lefts):
            l_buf[:, part * i:part * i + part] = ref[0]

    for i, ref in enumerate(rights):
        r_buf[part * i:part * i + part, :] = ref[...]

    sub = 512

    def body(i, carry):
        rows = pl.ds(pl.multiple_of(i * sub, sub), sub)
        tile = dot(l_buf[rows, :], r_buf[...])
        if flip:
            out_ref[:, rows] = tile.T
        elif add:
            out_ref[rows, :] = refs[2 * count][rows, :] + tile
        else:
            out_ref[rows, :] = tile
        return carry

    lax.fori_loop(0, l_buf.shape[0] // sub, body, 0)


def grad_call(lefts, rights, which, n_out, col, buf=None, flip=False, add=False):
    count = len(lefts)
    _, rows, part = lefts[0].shape
    n = rights[0].shape[1]
    tm, tn = 1024, 512
    specs = [pl.BlockSpec((1, tm, part), lambda i, j: (which, i, 0))] * count + [pl.BlockSpec((part, tn), lambda i, j: (0, j))] * count
    args = list(lefts) + list(rights)
    if flip:
        out_spec = pl.BlockSpec((tn, tm), lambda i, j: (j, i))
        out_shape = jax.ShapeDtypeStruct((n, rows), F32)
    else:
        out_spec = pl.BlockSpec((tm, tn), lambda i, j: (i, col // tn + j))
        out_shape = jax.ShapeDtypeStruct((rows, n_out), F32)
    aliases = {}
    if buf is not None:
        specs.append(out_spec if add else pl.BlockSpec(memory_space=pl.ANY))
        args.append(buf)
        aliases = {2 * count: 0}
    return pl.pallas_call(
        functools.partial(grad_kernel, count, flip, add),
        grid=(rows // tm, n // tn),
        in_specs=specs,
        out_specs=out_spec,
        out_shape=out_shape,
        scratch_shapes=[pltpu.VMEM((tm, part * count), BF16), pltpu.VMEM((part * count, tn), BF16)],
        input_output_aliases=aliases,
        compiler_params=pltpu.CompilerParams(dimension_semantics=("arbitrary",) * 2, vmem_limit_bytes=56 << 20),
        cost_estimate=pl.CostEstimate(flops=2 * rows * n * part * count, bytes_accessed=80_000_000, transcendentals=0),
        name="wgrad",
    )(*args)


def solution(mesh):
    def device_fn(x_in, positions, long_factor, norm_gain, w_qkv, w_out, grad_y):
        _, piece, hidden = x_in.shape
        n_dev = mesh.shape['cp']
        seq = piece * n_dev
        width = w_out.shape[0]
        scale = 1.0 / math.sqrt(2 * long_factor.shape[0])
        me = lax.axis_index('cp')
        mine = jnp.bitwise_xor(me, jnp.arange(n_dev))

        def shift(t, bit):
            return lax.ppermute(t, 'cp', [(i, i ^ bit) for i in range(n_dev)])

        def swap(t):
            sent = t[mine]
            return jnp.stack([sent[0]] + [shift(sent[m], m) for m in range(1, n_dev)])[mine]

        def after(values, deps):
            return lax.optimization_barrier((values, deps))[0]

        x = swap(x_in).reshape(seq, hidden)
        dy = swap(grad_y).reshape(seq, hidden)
        pos = lax.all_gather(positions, 'cp', tiled=True)
        cos, sin = rope_tables(pos, long_factor)
        r, pair_a, pair_b = norm_call(x, dy, norm_gain[None, :])

        def near(ab):
            a, b = ab
            return [a, b, shift(a, 2), shift(b, 2), shift(a, 4), shift(b, 4)]

        def far(pieces, deps=()):
            pieces = after(pieces, deps)
            diag = [shift(pieces[2], 4), shift(pieces[5], 2)]
            return pieces + [shift(t, 1) for t in pieces], diag + [shift(t, 1) for t in diag]

        pair_part = near((pair_a, pair_b))
        out = block_call(x, r, dy, norm_gain[None, :], w_qkv, w_out, cos, sin, scale)
        y, dx, gg = out[:3]
        pair_near, pair_far = far(pair_part, (gg,))
        o_part = near(out[3:5])
        q_part = near(out[5:7])
        k_part = near(after(out[7:9], o_part))
        o_near, o_far = far(o_part)
        y_out = swap(y.reshape(n_dev, piece, hidden))
        grad_x = swap(dx.reshape(n_dev, piece, hidden))
        g_gain = lax.psum(gg[0], 'cp')
        g_wout = grad_call(pair_near + pair_far, o_near + o_far, 1, hidden, 0, flip=True)
        v_part = near(after(out[9:11], q_part))
        q_near, q_far = far(q_part, (g_wout,))
        g_wqkv = grad_call(pair_near + pair_far, q_near + q_far, 0, 3 * width, 0)
        k_near, k_far = far(k_part, (g_wqkv,))
        g_wqkv = grad_call(pair_near + pair_far, k_near + k_far, 0, 3 * width, width, g_wqkv)
        v_near, v_far = far(v_part, (g_wqkv,))
        g_wqkv = grad_call(pair_near, v_near, 0, 3 * width, 2 * width, g_wqkv)
        g_wqkv = grad_call(pair_far, v_far, 0, 3 * width, 2 * width, g_wqkv, add=True)
        return y_out, grad_x, g_gain, g_wqkv, g_wout

    seq_spec = P('dp', 'cp', None)
    return jax.shard_map(device_fn, mesh=mesh, in_specs=(seq_spec, P(('dp', 'cp')), P(None), P(None), P(None, None), P(None, None), seq_spec), out_specs=(seq_spec, seq_spec, P('dp'), P('dp', None), P('dp', None)), check_vma=False)
```

```python
import functools
import math
import jax
import jax.numpy as jnp
from jax import lax
from jax.experimental import pallas as pl
from jax.experimental.pallas import tpu as pltpu
from jax.sharding import PartitionSpec as P

NORM_EPS = 1e-5
MSCALE = math.sqrt(1.0 + math.log(32.0) / math.log(4096.0))
MASK_VALUE = -1e30
F32 = jnp.float32
BF16 = jnp.bfloat16


def rope_tables(positions, long_factor):
    half = long_factor.shape[0]
    exponent = jnp.arange(half, dtype=F32) * (1.0 / half)
    inv_freq = 1.0 / (long_factor * jnp.power(10000.0, exponent))
    angles = positions.astype(F32)[:, None] * inv_freq[None, :]
    cos, sin = jnp.cos(angles) * MSCALE, jnp.sin(angles) * MSCALE
    return jnp.concatenate([cos] * 4, axis=1), jnp.concatenate([-sin, sin, -sin, sin], axis=1)


def dot(a, b, dims=((1,), (0,))):
    return lax.dot_general(a, b, (dims, ((), ())), preferred_element_type=F32)


def partner(t, first_half):
    width = t.shape[-1]
    return jnp.where(first_half, pltpu.roll(t, width - 32, 1), pltpu.roll(t, 32, 1))


def block_kernel(scale, x_ref, r_ref, dy_ref, gain_ref, wq_ref, wk_ref, wv_ref, wo_ref, cos_ref, sin_ref,
                 y_ref, dx_ref, gg_ref, oa_ref, ob_ref, qa_ref, qb_ref, ka_ref, kb_ref, va_ref, vb_ref, y_acc, dn_acc):
    step = pl.program_id(0)
    seq = x_ref.shape[0]
    qb = 256

    @pl.when(step == 0)
    def _():
        y_acc[...] = x_ref[...].astype(F32)
        dn_acc[...] = jnp.zeros_like(dn_acc)

    r = r_ref[...]
    q_all = dot(r, wq_ref[...])
    k_all = dot(r, wk_ref[...])
    v_all = dot(r, wv_ref[...]).astype(BF16)
    da_all = dot(dy_ref[...], wo_ref[...], ((1,), (1,))).astype(BF16)
    cos, sin = cos_ref[...], sin_ref[...]
    lane = lax.broadcasted_iota(jnp.int32, (seq, 128), 1)
    first_half = (lane % 64) < 32
    head0 = lane < 64
    tri = lax.broadcasted_iota(jnp.int32, (qb, qb), 0) <= lax.broadcasted_iota(jnp.int32, (qb, qb), 1)
    zero_rows = jnp.zeros((64, seq), BF16)
    zero_pair = jnp.zeros((seq, 128), BF16)

    for pair in range(2):
        cols = slice(128 * pair, 128 * pair + 128)
        qf, kf = q_all[:, cols], k_all[:, cols]
        q = ((qf * cos + partner(qf, first_half) * sin).astype(BF16) * scale).astype(BF16)
        k = (kf * cos + partner(kf, first_half) * sin).astype(BF16)
        v, da = v_all[:, cols], da_all[:, cols]
        qt, kt, vt, dat = q.T, k.T, v.T, da.T
        ots, dqts = [], []
        dk_sum = [jnp.zeros((qb, 128), F32), jnp.zeros((qb, 128), F32)]
        dv_sum = [jnp.zeros((qb, 128), F32), jnp.zeros((qb, 128), F32)]
        for head in range(2):
            rows = slice(64 * head, 64 * head + 64)
            if head == 0:
                qt_h = jnp.concatenate([qt[rows], zero_rows], axis=0)
                dat_h = jnp.concatenate([dat[rows], zero_rows], axis=0)
                q_h = jnp.where(head0, q, zero_pair)
                da_h = jnp.where(head0, da, zero_pair)
            else:
                qt_h = jnp.concatenate([zero_rows, qt[rows]], axis=0)
                dat_h = jnp.concatenate([zero_rows, dat[rows]], axis=0)
                q_h = jnp.where(head0, zero_pair, q)
                da_h = jnp.where(head0, zero_pair, da)
            kt_h, vt_h = kt[rows], vt[rows]
            ot_b, dqt_b = [], []
            for blk in range(2):
                qs = slice(qb * blk, qb * blk + qb)
                nk = qb * (blk + 1)
                st = dot(k[:nk], qt_h[:, qs])
                if blk == 0:
                    st = jnp.where(tri, st, MASK_VALUE)
                else:
                    st = jnp.concatenate([st[:qb], jnp.where(tri, st[qb:], MASK_VALUE)], axis=0)
                m = jnp.max(st, axis=0, keepdims=True)
                e = jnp.exp(st - m)
                p = e * (1.0 / jnp.sum(e, axis=0, keepdims=True))
                pb = p.astype(BF16)
                ot = dot(vt_h[:, :nk], pb)
                ob = ot.astype(BF16)
                delta = jnp.sum(dat[rows, qs].astype(F32) * ob.astype(F32), axis=0, keepdims=True)
                dpt = dot(v[:nk], dat_h[:, qs])
                dsb = (p * (dpt - delta)).astype(BF16)
                dqt_b.append(dot(kt_h[:, :nk], dsb))
                ot_b.append(ob)
                dv_part = dot(pb, da_h[qs])
                dk_part = dot(dsb, q_h[qs])
                for half in range(blk + 1):
                    hs = slice(qb * half, qb * half + qb)
                    dv_sum[half] += dv_part[hs]
                    dk_sum[half] += dk_part[hs]
            ots.append(jnp.concatenate(ot_b, axis=1))
            dqts.append(jnp.concatenate(dqt_b, axis=1))
        ot_pair = jnp.concatenate(ots, axis=0)
        o = ot_pair.T
        dq = jnp.concatenate(dqts, axis=0).T * scale
        dk = jnp.concatenate(dk_sum, axis=0)
        dv = jnp.concatenate(dv_sum, axis=0)
        dqb = (dq * cos - partner(dq, first_half) * sin).astype(BF16)
        dkb = (dk * cos - partner(dk, first_half) * sin).astype(BF16)
        dvb = dv.astype(BF16)
        for value, a_ref, b_ref in ((o, oa_ref, ob_ref), (dqb, qa_ref, qb_ref), (dkb, ka_ref, kb_ref), (dvb, va_ref, vb_ref)):
            a_ref[:, cols] = value[:qb]
            b_ref[:, cols] = value[qb:]
        y_acc[...] += dot(o, wo_ref[cols, :])

    for rows, dq_ref, dk_ref, dv_ref in ((slice(0, qb), qa_ref, ka_ref, va_ref), (slice(qb, 2 * qb), qb_ref, kb_ref, vb_ref)):
        dn_acc[rows, :] += (dot(dq_ref[...], wq_ref[...], ((1,), (1,))) + dot(dk_ref[...], wk_ref[...], ((1,), (1,)))
                            + dot(dv_ref[...], wv_ref[...], ((1,), (1,))))

    @pl.when(step == pl.num_programs(0) - 1)
    def _():
        y_ref[...] = y_acc[...].astype(BF16)
        x = x_ref[...].astype(F32)
        inv = lax.rsqrt(jnp.mean(x * x, axis=1, keepdims=True) + NORM_EPS)
        x_hat = x * inv
        dn = dn_acc[...]
        gg_ref[...] = jnp.sum(dn * x_hat, axis=0, keepdims=True)
        d_hat = dn * gain_ref[...]
        dx = inv * (d_hat - x_hat * jnp.mean(d_hat * x_hat, axis=1, keepdims=True))
        dx_ref[...] = (dy_ref[...].astype(F32) + dx).astype(BF16)


def block_call(x, r, dy, gain, w_qkv, w_out, cos, sin, scale):
    seq, hidden = x.shape
    width = w_out.shape[0]
    hb = 256
    steps = width // hb
    whole = lambda a: pl.BlockSpec(a.shape, lambda j: (0, 0), pipeline_mode=pl.Buffered(1))
    wcol = lambda part: pl.BlockSpec((hidden, hb), lambda j, part=part: (0, part * steps + j))
    tok = pl.BlockSpec((seq // 2, hb), lambda j: (0, j))
    full = lambda s: pl.BlockSpec(s, lambda j: (0, 0))
    return pl.pallas_call(
        functools.partial(block_kernel, scale),
        grid=(steps,),
        in_specs=[whole(x), whole(r), whole(dy), whole(gain), wcol(0), wcol(1), wcol(2),
                  pl.BlockSpec((hb, hidden), lambda j: (j, 0)), whole(cos), whole(sin)],
        out_specs=[full((seq, hidden)), full((seq, hidden)), full((1, hidden))] + [tok] * 8,
        out_shape=[jax.ShapeDtypeStruct((seq, hidden), BF16), jax.ShapeDtypeStruct((seq, hidden), BF16),
                   jax.ShapeDtypeStruct((1, hidden), F32)] + [jax.ShapeDtypeStruct((seq // 2, width), BF16)] * 8,
        scratch_shapes=[pltpu.VMEM((seq, hidden), F32), pltpu.VMEM((seq, hidden), F32)],
        compiler_params=pltpu.CompilerParams(dimension_semantics=("arbitrary",), vmem_limit_bytes=60 << 20),
        cost_estimate=pl.CostEstimate(flops=60_000_000_000, bytes_accessed=60_000_000, transcendentals=8_000_000),
        name="block",
    )(x, r, dy, gain, w_qkv, w_qkv, w_qkv, w_out, cos, sin)


def norm_kernel(both_ref, gain_ref, x_ref, dy_ref, r_ref, *pair_refs):
    n, rows, hidden = both_ref.shape
    piece = rows // 2
    xb = both_ref[:, :piece, :].reshape(n * piece, hidden)
    dy = both_ref[:, piece:, :].reshape(n * piece, hidden)
    x_ref[...] = xb
    dy_ref[...] = dy
    x = xb.astype(F32)
    inv = lax.rsqrt(jnp.mean(x * x, axis=1, keepdims=True) + NORM_EPS)
    r = (x * inv * gain_ref[...]).astype(BF16)
    r_ref[...] = r
    part = pair_refs[0].shape[2]
    for i, ref in enumerate(pair_refs):
        ref[0] = r[part * i:part * i + part].T
        ref[1] = dy[part * i:part * i + part].T


def norm_call(both, gain):
    n, rows, hidden = both.shape
    seq = n * rows // 2
    return pl.pallas_call(
        norm_kernel,
        out_shape=[jax.ShapeDtypeStruct((seq, hidden), BF16)] * 3 + [jax.ShapeDtypeStruct((2, hidden, seq // 2), BF16)] * 2,
        compiler_params=pltpu.CompilerParams(vmem_limit_bytes=48 << 20),
        cost_estimate=pl.CostEstimate(flops=10_000_000, bytes_accessed=14_000_000, transcendentals=0),
        name="norm",
    )(both, gain)


def grad_kernel(count, flip, add, *refs):
    lefts, rights = refs[:count], refs[count:2 * count]
    out_ref, l_buf, r_buf = refs[-3:]
    part = lefts[0].shape[2]

    @pl.when(pl.program_id(1) == 0)
    def _():
        for i, ref in enumerate(lefts):
            l_buf[:, part * i:part * i + part] = ref[0]

    for i, ref in enumerate(rights):
        r_buf[part * i:part * i + part, :] = ref[...]

    sub = 512

    def body(i, carry):
        rows = pl.ds(pl.multiple_of(i * sub, sub), sub)
        tile = dot(l_buf[rows, :], r_buf[...])
        if flip:
            out_ref[:, rows] = tile.T
        elif add:
            out_ref[rows, :] = refs[2 * count][rows, :] + tile
        else:
            out_ref[rows, :] = tile
        return carry

    lax.fori_loop(0, l_buf.shape[0] // sub, body, 0)


def grad_call(lefts, rights, which, n_out, col, buf=None, flip=False, add=False):
    count = len(lefts)
    _, rows, part = lefts[0].shape
    n = rights[0].shape[1]
    tm, tn = 1024, 512
    specs = [pl.BlockSpec((1, tm, part), lambda i, j: (which, i, 0))] * count + [pl.BlockSpec((part, tn), lambda i, j: (0, j))] * count
    args = list(lefts) + list(rights)
    if flip:
        out_spec = pl.BlockSpec((tn, tm), lambda i, j: (j, i))
        out_shape = jax.ShapeDtypeStruct((n, rows), F32)
    else:
        out_spec = pl.BlockSpec((tm, tn), lambda i, j: (i, col // tn + j))
        out_shape = jax.ShapeDtypeStruct((rows, n_out), F32)
    aliases = {}
    if buf is not None:
        specs.append(out_spec if add else pl.BlockSpec(memory_space=pl.ANY))
        args.append(buf)
        aliases = {2 * count: 0}
    return pl.pallas_call(
        functools.partial(grad_kernel, count, flip, add),
        grid=(rows // tm, n // tn),
        in_specs=specs,
        out_specs=out_spec,
        out_shape=out_shape,
        scratch_shapes=[pltpu.VMEM((tm, part * count), BF16), pltpu.VMEM((part * count, tn), BF16)],
        input_output_aliases=aliases,
        compiler_params=pltpu.CompilerParams(dimension_semantics=("arbitrary",) * 2, vmem_limit_bytes=56 << 20),
        cost_estimate=pl.CostEstimate(flops=2 * rows * n * part * count, bytes_accessed=80_000_000, transcendentals=0),
        name="wgrad",
    )(*args)


def solution(mesh):
    def device_fn(x_in, positions, long_factor, norm_gain, w_qkv, w_out, grad_y):
        _, piece, hidden = x_in.shape
        n_dev = mesh.shape['cp']
        width = w_out.shape[0]
        scale = 1.0 / math.sqrt(2 * long_factor.shape[0])
        me = lax.axis_index('cp')
        mine = jnp.bitwise_xor(me, jnp.arange(n_dev))

        def shift(t, bit):
            return lax.ppermute(t, 'cp', [(i, i ^ bit) for i in range(n_dev)])

        def swap(t):
            sent = t[mine]
            return jnp.stack([sent[0]] + [shift(sent[m], m) for m in range(1, n_dev)])[mine]

        def after(values, deps):
            return lax.optimization_barrier((values, deps))[0]

        both = lax.all_to_all(jnp.concatenate([x_in, grad_y], axis=1), 'cp', split_axis=0, concat_axis=0)
        pos = lax.all_gather(positions, 'cp', tiled=True)
        cos, sin = rope_tables(pos, long_factor)
        x, dy, r, pair_a, pair_b = norm_call(both, norm_gain[None, :])

        def near(ab):
            a, b = ab
            return [a, b, shift(a, 2), shift(b, 2), shift(a, 4), shift(b, 4)]

        def far(pieces, deps=()):
            pieces = after(pieces, deps)
            diag = [shift(pieces[2], 4), shift(pieces[5], 2)]
            return pieces + [shift(t, 1) for t in pieces], diag + [shift(t, 1) for t in diag]

        pair_part = near((pair_a, pair_b))
        out = block_call(x, r, dy, norm_gain[None, :], w_qkv, w_out, cos, sin, scale)
        y, dx, gg = out[:3]
        pair_near, pair_far = far(pair_part, (gg,))
        o_part = near(out[3:5])
        q_part = near(out[5:7])
        k_part = near(after(out[7:9], o_part))
        o_near, o_far = far(o_part)
        gg1 = shift(gg, 1)
        g_wout = grad_call(pair_near + pair_far, o_near + o_far, 1, hidden, 0, flip=True)
        y_out = swap(after(y, g_wout).reshape(n_dev, piece, hidden))
        gg, gg1 = after((gg, gg1), g_wout)
        gg = gg + gg1
        gg2 = shift(gg, 2)
        v_part = near(after(out[9:11], q_part))
        q_near, q_far = far(q_part, (g_wout,))
        g_wqkv = grad_call(pair_near + pair_far, q_near + q_far, 0, 3 * width, 0)
        grad_x = swap(after(dx, g_wqkv).reshape(n_dev, piece, hidden))
        gg, gg2 = after((gg, gg2), g_wqkv)
        gg = gg + gg2
        gg4 = shift(gg, 4)
        k_near, k_far = far(k_part, (g_wqkv,))
        g_wqkv = grad_call(pair_near + pair_far, k_near + k_far, 0, 3 * width, width, g_wqkv)
        gg, gg4 = after((gg, gg4), g_wqkv)
        g_gain = (gg + gg4)[0]
        v_near, v_far = far(v_part, (g_wqkv,))
        g_wqkv = grad_call(pair_near, v_near, 0, 3 * width, 2 * width, g_wqkv)
        g_wqkv = grad_call(pair_far, v_far, 0, 3 * width, 2 * width, g_wqkv, add=True)
        return y_out, grad_x, g_gain, g_wqkv, g_wout

    seq_spec = P('dp', 'cp', None)
    return jax.shard_map(device_fn, mesh=mesh, in_specs=(seq_spec, P(('dp', 'cp')), P(None), P(None), P(None, None), P(None, None), seq_spec), out_specs=(seq_spec, seq_spec, P('dp'), P('dp', None), P('dp', None)), check_vma=False)
```

```python
import functools
import math
import jax
import jax.numpy as jnp
from jax import lax
from jax.experimental import pallas as pl
from jax.experimental.pallas import tpu as pltpu
from jax.sharding import PartitionSpec as P

NORM_EPS = 1e-5
MSCALE = math.sqrt(1.0 + math.log(32.0) / math.log(4096.0))
MASK_VALUE = -1e30
F32 = jnp.float32
BF16 = jnp.bfloat16


def rope_tables(positions, long_factor):
    half = long_factor.shape[0]
    exponent = jnp.arange(half, dtype=F32) * (1.0 / half)
    inv_freq = 1.0 / (long_factor * jnp.power(10000.0, exponent))
    angles = positions.astype(F32)[:, None] * inv_freq[None, :]
    cos, sin = jnp.cos(angles) * MSCALE, jnp.sin(angles) * MSCALE
    return jnp.concatenate([cos] * 4, axis=1), jnp.concatenate([-sin, sin, -sin, sin], axis=1)


def dot(a, b, dims=((1,), (0,))):
    return lax.dot_general(a, b, (dims, ((), ())), preferred_element_type=F32)


def partner(t, first_half):
    width = t.shape[-1]
    return jnp.where(first_half, pltpu.roll(t, width - 32, 1), pltpu.roll(t, 32, 1))


def block_kernel(scale, me_ref, x_ref, r_ref, dy_ref, gain_ref, wq_ref, wk_ref, wv_ref, wo_ref, cos_ref, sin_ref,
                 gg_ref, oa_ref, ob_ref, qa_ref, qb_ref, ka_ref, kb_ref, va_ref, vb_ref, *rest):
    back_refs, (y_acc, dn_acc) = rest[:-2], rest[-2:]
    step = pl.program_id(0)
    seq = x_ref.shape[0]
    qb = 256

    @pl.when(step == 0)
    def _():
        y_acc[...] = x_ref[...].astype(F32)
        dn_acc[...] = jnp.zeros_like(dn_acc)

    r = r_ref[...]
    q_all = dot(r, wq_ref[...])
    k_all = dot(r, wk_ref[...])
    v_all = dot(r, wv_ref[...]).astype(BF16)
    da_all = dot(dy_ref[...], wo_ref[...], ((1,), (1,))).astype(BF16)
    cos, sin = cos_ref[...], sin_ref[...]
    lane = lax.broadcasted_iota(jnp.int32, (seq, 128), 1)
    first_half = (lane % 64) < 32
    head0 = lane < 64
    tri = lax.broadcasted_iota(jnp.int32, (qb, qb), 0) <= lax.broadcasted_iota(jnp.int32, (qb, qb), 1)
    zero_rows = jnp.zeros((64, seq), BF16)
    zero_pair = jnp.zeros((seq, 128), BF16)

    for pair in range(2):
        cols = slice(128 * pair, 128 * pair + 128)
        qf, kf = q_all[:, cols], k_all[:, cols]
        q = ((qf * cos + partner(qf, first_half) * sin).astype(BF16) * scale).astype(BF16)
        k = (kf * cos + partner(kf, first_half) * sin).astype(BF16)
        v, da = v_all[:, cols], da_all[:, cols]
        qt, kt, vt, dat = q.T, k.T, v.T, da.T
        ots, dqts = [], []
        dk_sum = [jnp.zeros((qb, 128), F32), jnp.zeros((qb, 128), F32)]
        dv_sum = [jnp.zeros((qb, 128), F32), jnp.zeros((qb, 128), F32)]
        for head in range(2):
            rows = slice(64 * head, 64 * head + 64)
            if head == 0:
                qt_h = jnp.concatenate([qt[rows], zero_rows], axis=0)
                dat_h = jnp.concatenate([dat[rows], zero_rows], axis=0)
                q_h = jnp.where(head0, q, zero_pair)
                da_h = jnp.where(head0, da, zero_pair)
            else:
                qt_h = jnp.concatenate([zero_rows, qt[rows]], axis=0)
                dat_h = jnp.concatenate([zero_rows, dat[rows]], axis=0)
                q_h = jnp.where(head0, zero_pair, q)
                da_h = jnp.where(head0, zero_pair, da)
            kt_h, vt_h = kt[rows], vt[rows]
            ot_b, dqt_b = [], []
            for blk in range(2):
                qs = slice(qb * blk, qb * blk + qb)
                nk = qb * (blk + 1)
                st = dot(k[:nk], qt_h[:, qs])
                if blk == 0:
                    st = jnp.where(tri, st, MASK_VALUE)
                else:
                    st = jnp.concatenate([st[:qb], jnp.where(tri, st[qb:], MASK_VALUE)], axis=0)
                m = jnp.max(st, axis=0, keepdims=True)
                e = jnp.exp(st - m)
                p = e * (1.0 / jnp.sum(e, axis=0, keepdims=True))
                pb = p.astype(BF16)
                ot = dot(vt_h[:, :nk], pb)
                ob = ot.astype(BF16)
                delta = jnp.sum(dat[rows, qs].astype(F32) * ob.astype(F32), axis=0, keepdims=True)
                dpt = dot(v[:nk], dat_h[:, qs])
                dsb = (p * (dpt - delta)).astype(BF16)
                dqt_b.append(dot(kt_h[:, :nk], dsb))
                ot_b.append(ob)
                dv_part = dot(pb, da_h[qs])
                dk_part = dot(dsb, q_h[qs])
                for half in range(blk + 1):
                    hs = slice(qb * half, qb * half + qb)
                    dv_sum[half] += dv_part[hs]
                    dk_sum[half] += dk_part[hs]
            ots.append(jnp.concatenate(ot_b, axis=1))
            dqts.append(jnp.concatenate(dqt_b, axis=1))
        ot_pair = jnp.concatenate(ots, axis=0)
        o = ot_pair.T
        dq = jnp.concatenate(dqts, axis=0).T * scale
        dk = jnp.concatenate(dk_sum, axis=0)
        dv = jnp.concatenate(dv_sum, axis=0)
        dqb = (dq * cos - partner(dq, first_half) * sin).astype(BF16)
        dkb = (dk * cos - partner(dk, first_half) * sin).astype(BF16)
        dvb = dv.astype(BF16)
        for value, a_ref, b_ref in ((o, oa_ref, ob_ref), (dqb, qa_ref, qb_ref), (dkb, ka_ref, kb_ref), (dvb, va_ref, vb_ref)):
            a_ref[:, cols] = value[:qb]
            b_ref[:, cols] = value[qb:]
        y_acc[...] += dot(o, wo_ref[cols, :])

    for rows, dq_ref, dk_ref, dv_ref in ((slice(0, qb), qa_ref, ka_ref, va_ref), (slice(qb, 2 * qb), qb_ref, kb_ref, vb_ref)):
        dn_acc[rows, :] += (dot(dq_ref[...], wq_ref[...], ((1,), (1,))) + dot(dk_ref[...], wk_ref[...], ((1,), (1,)))
                            + dot(dv_ref[...], wv_ref[...], ((1,), (1,))))

    @pl.when(step == pl.num_programs(0) - 1)
    def _():
        x = x_ref[...].astype(F32)
        inv = lax.rsqrt(jnp.mean(x * x, axis=1, keepdims=True) + NORM_EPS)
        x_hat = x * inv
        dn = dn_acc[...]
        gg_ref[...] = jnp.sum(dn * x_hat, axis=0, keepdims=True)
        d_hat = dn * gain_ref[...]
        dx = inv * (d_hat - x_hat * jnp.mean(d_hat * x_hat, axis=1, keepdims=True))
        dn_acc[...] = dy_ref[...].astype(F32) + dx
        piece = back_refs[0].shape[1]
        for m, ref in enumerate(back_refs):
            rows = pl.ds(pl.multiple_of(jnp.bitwise_xor(me_ref[0], m) * piece, piece), piece)
            ref[0] = y_acc[rows, :].astype(BF16)
            ref[1] = dn_acc[rows, :].astype(BF16)


def block_call(me, x, r, dy, gain, w_qkv, w_out, cos, sin, scale, n_dev):
    seq, hidden = x.shape
    width = w_out.shape[0]
    hb = 256
    steps = width // hb
    whole = lambda a: pl.BlockSpec(a.shape, lambda j: (0, 0), pipeline_mode=pl.Buffered(1))
    wcol = lambda part: pl.BlockSpec((hidden, hb), lambda j, part=part: (0, part * steps + j))
    tok = pl.BlockSpec((seq // 2, hb), lambda j: (0, j))
    full = lambda s: pl.BlockSpec(s, lambda j: (0, 0))
    back = (2, seq // n_dev, hidden)
    return pl.pallas_call(
        functools.partial(block_kernel, scale),
        grid=(steps,),
        in_specs=[pl.BlockSpec(memory_space=pltpu.SMEM), whole(x), whole(r), whole(dy), whole(gain), wcol(0), wcol(1), wcol(2),
                  pl.BlockSpec((hb, hidden), lambda j: (j, 0)), whole(cos), whole(sin)],
        out_specs=[full((1, hidden))] + [tok] * 8 + [pl.BlockSpec(back, lambda j: (0, 0, 0))] * n_dev,
        out_shape=[jax.ShapeDtypeStruct((1, hidden), F32)] + [jax.ShapeDtypeStruct((seq // 2, width), BF16)] * 8
        + [jax.ShapeDtypeStruct(back, BF16)] * n_dev,
        scratch_shapes=[pltpu.VMEM((seq, hidden), F32), pltpu.VMEM((seq, hidden), F32)],
        compiler_params=pltpu.CompilerParams(dimension_semantics=("arbitrary",), vmem_limit_bytes=60 << 20),
        cost_estimate=pl.CostEstimate(flops=60_000_000_000, bytes_accessed=60_000_000, transcendentals=8_000_000),
        name="block",
    )(me, x, r, dy, gain, w_qkv, w_qkv, w_qkv, w_out, cos, sin)


def join_kernel(me_ref, *refs):
    y_ref, dx_ref = refs[-2:]
    for m, ref in enumerate(refs[:-2]):
        owner = jnp.bitwise_xor(me_ref[0], m)
        y_ref[owner] = ref[0]
        dx_ref[owner] = ref[1]


def join_call(me, parts):
    n_dev = len(parts)
    _, piece, hidden = parts[0].shape
    return pl.pallas_call(
        join_kernel,
        in_specs=[pl.BlockSpec(memory_space=pltpu.SMEM)] + [pl.BlockSpec(memory_space=pltpu.VMEM)] * n_dev,
        out_shape=[jax.ShapeDtypeStruct((n_dev, piece, hidden), BF16)] * 2,
        compiler_params=pltpu.CompilerParams(vmem_limit_bytes=32 << 20),
        cost_estimate=pl.CostEstimate(flops=1_000_000, bytes_accessed=8_000_000, transcendentals=0),
        name="join",
    )(me, *parts)


def norm_kernel(both_ref, gain_ref, x_ref, dy_ref, r_ref, *pair_refs):
    n, rows, hidden = both_ref.shape
    piece = rows // 2
    xb = both_ref[:, :piece, :].reshape(n * piece, hidden)
    dy = both_ref[:, piece:, :].reshape(n * piece, hidden)
    x_ref[...] = xb
    dy_ref[...] = dy
    x = xb.astype(F32)
    inv = lax.rsqrt(jnp.mean(x * x, axis=1, keepdims=True) + NORM_EPS)
    r = (x * inv * gain_ref[...]).astype(BF16)
    r_ref[...] = r
    part = pair_refs[0].shape[2]
    for i, ref in enumerate(pair_refs):
        ref[0] = r[part * i:part * i + part].T
        ref[1] = dy[part * i:part * i + part].T


def norm_call(both, gain):
    n, rows, hidden = both.shape
    seq = n * rows // 2
    return pl.pallas_call(
        norm_kernel,
        out_shape=[jax.ShapeDtypeStruct((seq, hidden), BF16)] * 3 + [jax.ShapeDtypeStruct((2, hidden, seq // 2), BF16)] * 2,
        compiler_params=pltpu.CompilerParams(vmem_limit_bytes=48 << 20),
        cost_estimate=pl.CostEstimate(flops=10_000_000, bytes_accessed=14_000_000, transcendentals=0),
        name="norm",
    )(both, gain)


def grad_kernel(count, flip, add, *refs):
    lefts, rights = refs[:count], refs[count:2 * count]
    out_ref, l_buf, r_buf = refs[-3:]
    part = lefts[0].shape[2]

    @pl.when(pl.program_id(1) == 0)
    def _():
        for i, ref in enumerate(lefts):
            l_buf[:, part * i:part * i + part] = ref[0]

    for i, ref in enumerate(rights):
        r_buf[part * i:part * i + part, :] = ref[...]

    sub = 512

    def body(i, carry):
        rows = pl.ds(pl.multiple_of(i * sub, sub), sub)
        tile = dot(l_buf[rows, :], r_buf[...])
        if flip and add:
            out_ref[:, rows] = refs[2 * count][:, rows] + tile.T
        elif flip:
            out_ref[:, rows] = tile.T
        elif add:
            out_ref[rows, :] = refs[2 * count][rows, :] + tile
        else:
            out_ref[rows, :] = tile
        return carry

    lax.fori_loop(0, l_buf.shape[0] // sub, body, 0)


def grad_call(lefts, rights, which, n_out, col, buf=None, flip=False, add=False):
    count = len(lefts)
    _, rows, part = lefts[0].shape
    n = rights[0].shape[1]
    tm, tn = 1024, 512
    specs = [pl.BlockSpec((1, tm, part), lambda i, j: (which, i, 0))] * count + [pl.BlockSpec((part, tn), lambda i, j: (0, j))] * count
    args = list(lefts) + list(rights)
    if flip:
        out_spec = pl.BlockSpec((tn, tm), lambda i, j: (j, i))
        out_shape = jax.ShapeDtypeStruct((n, rows), F32)
    else:
        out_spec = pl.BlockSpec((tm, tn), lambda i, j: (i, col // tn + j))
        out_shape = jax.ShapeDtypeStruct((rows, n_out), F32)
    aliases = {}
    if buf is not None:
        specs.append(out_spec if add else pl.BlockSpec(memory_space=pl.ANY))
        args.append(buf)
        aliases = {2 * count: 0}
    return pl.pallas_call(
        functools.partial(grad_kernel, count, flip, add),
        grid=(rows // tm, n // tn),
        in_specs=specs,
        out_specs=out_spec,
        out_shape=out_shape,
        scratch_shapes=[pltpu.VMEM((tm, part * count), BF16), pltpu.VMEM((part * count, tn), BF16)],
        input_output_aliases=aliases,
        compiler_params=pltpu.CompilerParams(dimension_semantics=("arbitrary",) * 2, vmem_limit_bytes=56 << 20),
        cost_estimate=pl.CostEstimate(flops=2 * rows * n * part * count, bytes_accessed=80_000_000, transcendentals=0),
        name="wgrad",
    )(*args)


def solution(mesh):
    def device_fn(x_in, positions, long_factor, norm_gain, w_qkv, w_out, grad_y):
        _, _, hidden = x_in.shape
        n_dev = mesh.shape['cp']
        width = w_out.shape[0]
        scale = 1.0 / math.sqrt(2 * long_factor.shape[0])
        me = lax.axis_index('cp').astype(jnp.int32)[None]

        def shift(t, bit):
            return lax.ppermute(t, 'cp', [(i, i ^ bit) for i in range(n_dev)])

        def after(values, deps):
            return lax.optimization_barrier((values, deps))[0]

        both = lax.all_to_all(jnp.concatenate([x_in, grad_y], axis=1), 'cp', split_axis=0, concat_axis=0)
        pos = lax.all_gather(positions, 'cp', tiled=True)
        cos, sin = rope_tables(pos, long_factor)
        x, dy, r, pair_a, pair_b = norm_call(both, norm_gain[None, :])

        def own(ab):
            a, b = ab
            return [a, b, shift(a, 1), shift(b, 1)]

        def near(ab):
            a, b = ab
            return [shift(a, 2), shift(b, 2), shift(a, 4), shift(b, 4)]

        def far(part, deps=()):
            part = after(part, deps)
            diag = [shift(part[0], 4), shift(part[3], 2)]
            every = list(part) + diag
            return every + [shift(t, 1) for t in every]

        p_ab = (pair_a, pair_b)
        p_part, p_own = near(p_ab), own(p_ab)
        out = block_call(me, x, r, dy, norm_gain[None, :], w_qkv, w_out, cos, sin, scale, n_dev)
        gg = out[0]
        o_ab, q_ab, k_ab, v_ab = (tuple(out[i:i + 2]) for i in (1, 3, 5, 7))
        back = out[9:]
        gg1 = shift(gg, 1)
        p_rest = far(p_part, (gg,))
        o_part = near(o_ab)
        cols = 3 * width
        g_wout = grad_call(p_own, own(o_ab), 1, hidden, 0, flip=True)
        g_wqkv = grad_call(p_own, own(q_ab), 0, cols, 0)
        g_wqkv = grad_call(p_own, own(k_ab), 0, cols, width, g_wqkv)
        g_wqkv = grad_call(p_own, own(v_ab), 0, cols, 2 * width, g_wqkv)
        gg, gg1 = after((gg, gg1), g_wqkv)
        gg = gg + gg1
        o_rest = far(o_part, (g_wqkv, g_wout))
        gg2 = shift(gg, 2)
        q_part = near(after(q_ab, o_part))
        k_part = near(after(k_ab, o_part))
        g_wout = grad_call(p_rest, o_rest, 1, hidden, 0, g_wout, flip=True, add=True)
        gg, gg2 = after((gg, gg2), g_wout)
        gg = gg + gg2
        q_rest = far(q_part, (g_wout,))
        gg4 = shift(gg, 4)
        v_part = near(after(v_ab, q_part))
        k_rest = far(k_part, (g_wout,))
        g_wqkv = grad_call(p_rest, q_rest, 0, cols, 0, g_wqkv, add=True)
        gg, gg4 = after((gg, gg4), g_wqkv)
        g_gain = (gg + gg4)[0]
        v_rest = far(v_part, (g_wqkv,))
        back = [back[0]] + [shift(t, m + 1) for m, t in enumerate(after(back[1:], g_wqkv))]
        g_wqkv = grad_call(p_rest, k_rest, 0, cols, width, g_wqkv, add=True)
        g_wqkv = grad_call(p_rest, v_rest, 0, cols, 2 * width, g_wqkv, add=True)
        y_out, grad_x = join_call(*after((me, back), g_wqkv))
        return y_out, grad_x, g_gain, g_wqkv, g_wout

    seq_spec = P('dp', 'cp', None)
    return jax.shard_map(device_fn, mesh=mesh, in_specs=(seq_spec, P(('dp', 'cp')), P(None), P(None), P(None, None), P(None, None), seq_spec), out_specs=(seq_spec, seq_spec, P('dp'), P('dp', None), P('dp', None)), check_vma=False)
```

```python
import functools
import math
import jax
import jax.numpy as jnp
from jax import lax
from jax.experimental import pallas as pl
from jax.experimental.pallas import tpu as pltpu
from jax.sharding import PartitionSpec as P

NORM_EPS = 1e-5
MSCALE = math.sqrt(1.0 + math.log(32.0) / math.log(4096.0))
MASK_VALUE = -1e30
F32 = jnp.float32
BF16 = jnp.bfloat16


def rope_tables(positions, long_factor):
    half = long_factor.shape[0]
    exponent = jnp.arange(half, dtype=F32) * (1.0 / half)
    inv_freq = 1.0 / (long_factor * jnp.power(10000.0, exponent))
    angles = positions.astype(F32)[:, None] * inv_freq[None, :]
    cos, sin = jnp.cos(angles) * MSCALE, jnp.sin(angles) * MSCALE
    return jnp.concatenate([cos] * 4, axis=1), jnp.concatenate([-sin, sin, -sin, sin], axis=1)


def dot(a, b, dims=((1,), (0,))):
    return lax.dot_general(a, b, (dims, ((), ())), preferred_element_type=F32)


def partner(t, first_half):
    width = t.shape[-1]
    return jnp.where(first_half, pltpu.roll(t, width - 32, 1), pltpu.roll(t, 32, 1))


def block_kernel(scale, me_ref, x_ref, r_ref, dy_ref, gain_ref, wq_ref, wk_ref, wv_ref, wo_ref, cos_ref, sin_ref,
                 gg_ref, oa_ref, ob_ref, qa_ref, qb_ref, ka_ref, kb_ref, va_ref, vb_ref, *rest):
    back_refs, (y_acc, dn_acc) = rest[:-2], rest[-2:]
    step = pl.program_id(0)
    seq = x_ref.shape[0]
    qb = 256

    @pl.when(step == 0)
    def _():
        y_acc[...] = x_ref[...].astype(F32)
        dn_acc[...] = jnp.zeros_like(dn_acc)

    r = r_ref[...]
    q_all = dot(r, wq_ref[...])
    k_all = dot(r, wk_ref[...])
    v_all = dot(r, wv_ref[...]).astype(BF16)
    da_all = dot(dy_ref[...], wo_ref[...], ((1,), (1,))).astype(BF16)
    cos, sin = cos_ref[...], sin_ref[...]
    lane = lax.broadcasted_iota(jnp.int32, (seq, 128), 1)
    first_half = (lane % 64) < 32
    head0 = lane < 64
    tri = lax.broadcasted_iota(jnp.int32, (qb, qb), 0) <= lax.broadcasted_iota(jnp.int32, (qb, qb), 1)
    zero_rows = jnp.zeros((64, seq), BF16)
    zero_pair = jnp.zeros((seq, 128), BF16)

    for pair in range(2):
        cols = slice(128 * pair, 128 * pair + 128)
        qf, kf = q_all[:, cols], k_all[:, cols]
        q = ((qf * cos + partner(qf, first_half) * sin).astype(BF16) * scale).astype(BF16)
        k = (kf * cos + partner(kf, first_half) * sin).astype(BF16)
        v, da = v_all[:, cols], da_all[:, cols]
        qt, kt, vt, dat = q.T, k.T, v.T, da.T
        ots, dqts = [], []
        dk_sum = [jnp.zeros((qb, 128), F32), jnp.zeros((qb, 128), F32)]
        dv_sum = [jnp.zeros((qb, 128), F32), jnp.zeros((qb, 128), F32)]
        for head in range(2):
            rows = slice(64 * head, 64 * head + 64)
            if head == 0:
                qt_h = jnp.concatenate([qt[rows], zero_rows], axis=0)
                dat_h = jnp.concatenate([dat[rows], zero_rows], axis=0)
                q_h = jnp.where(head0, q, zero_pair)
                da_h = jnp.where(head0, da, zero_pair)
            else:
                qt_h = jnp.concatenate([zero_rows, qt[rows]], axis=0)
                dat_h = jnp.concatenate([zero_rows, dat[rows]], axis=0)
                q_h = jnp.where(head0, zero_pair, q)
                da_h = jnp.where(head0, zero_pair, da)
            kt_h, vt_h = kt[rows], vt[rows]
            ot_b, dqt_b = [], []
            for blk in range(2):
                qs = slice(qb * blk, qb * blk + qb)
                nk = qb * (blk + 1)
                st = dot(k[:nk], qt_h[:, qs])
                if blk == 0:
                    st = jnp.where(tri, st, MASK_VALUE)
                else:
                    st = jnp.concatenate([st[:qb], jnp.where(tri, st[qb:], MASK_VALUE)], axis=0)
                m = jnp.max(st, axis=0, keepdims=True)
                e = jnp.exp(st - m)
                p = e * (1.0 / jnp.sum(e, axis=0, keepdims=True))
                pb = p.astype(BF16)
                ot = dot(vt_h[:, :nk], pb)
                ob = ot.astype(BF16)
                delta = jnp.sum(dat[rows, qs].astype(F32) * ob.astype(F32), axis=0, keepdims=True)
                dpt = dot(v[:nk], dat_h[:, qs])
                dsb = (p * (dpt - delta)).astype(BF16)
                dqt_b.append(dot(kt_h[:, :nk], dsb))
                ot_b.append(ob)
                dv_part = dot(pb, da_h[qs])
                dk_part = dot(dsb, q_h[qs])
                for half in range(blk + 1):
                    hs = slice(qb * half, qb * half + qb)
                    dv_sum[half] += dv_part[hs]
                    dk_sum[half] += dk_part[hs]
            ots.append(jnp.concatenate(ot_b, axis=1))
            dqts.append(jnp.concatenate(dqt_b, axis=1))
        ot_pair = jnp.concatenate(ots, axis=0)
        o = ot_pair.T
        dq = jnp.concatenate(dqts, axis=0).T * scale
        dk = jnp.concatenate(dk_sum, axis=0)
        dv = jnp.concatenate(dv_sum, axis=0)
        dqb = (dq * cos - partner(dq, first_half) * sin).astype(BF16)
        dkb = (dk * cos - partner(dk, first_half) * sin).astype(BF16)
        dvb = dv.astype(BF16)
        for value, a_ref, b_ref in ((o, oa_ref, ob_ref), (dqb, qa_ref, qb_ref), (dkb, ka_ref, kb_ref), (dvb, va_ref, vb_ref)):
            a_ref[:, cols] = value[:qb]
            b_ref[:, cols] = value[qb:]
        y_acc[...] += dot(o, wo_ref[cols, :])

    for rows, dq_ref, dk_ref, dv_ref in ((slice(0, qb), qa_ref, ka_ref, va_ref), (slice(qb, 2 * qb), qb_ref, kb_ref, vb_ref)):
        dn_acc[rows, :] += (dot(dq_ref[...], wq_ref[...], ((1,), (1,))) + dot(dk_ref[...], wk_ref[...], ((1,), (1,)))
                            + dot(dv_ref[...], wv_ref[...], ((1,), (1,))))

    @pl.when(step == pl.num_programs(0) - 1)
    def _():
        x = x_ref[...].astype(F32)
        inv = lax.rsqrt(jnp.mean(x * x, axis=1, keepdims=True) + NORM_EPS)
        x_hat = x * inv
        dn = dn_acc[...]
        gg_ref[...] = jnp.sum(dn * x_hat, axis=0, keepdims=True)
        d_hat = dn * gain_ref[...]
        dx = inv * (d_hat - x_hat * jnp.mean(d_hat * x_hat, axis=1, keepdims=True))
        dn_acc[...] = dy_ref[...].astype(F32) + dx
        piece = back_refs[0].shape[1]
        for m, ref in enumerate(back_refs):
            rows = pl.ds(pl.multiple_of(jnp.bitwise_xor(me_ref[0], m) * piece, piece), piece)
            ref[0] = y_acc[rows, :].astype(BF16)
            ref[1] = dn_acc[rows, :].astype(BF16)


def block_call(me, x, r, dy, gain, w_qkv, w_out, cos, sin, scale, n_dev):
    seq, hidden = x.shape
    width = w_out.shape[0]
    hb = 256
    steps = width // hb
    whole = lambda a: pl.BlockSpec(a.shape, lambda j: (0, 0), pipeline_mode=pl.Buffered(1))
    wcol = lambda part: pl.BlockSpec((hidden, hb), lambda j, part=part: (0, part * steps + j))
    tok = pl.BlockSpec((seq // 2, hb), lambda j: (0, j))
    full = lambda s: pl.BlockSpec(s, lambda j: (0, 0))
    back = (2, seq // n_dev, hidden)
    return pl.pallas_call(
        functools.partial(block_kernel, scale),
        grid=(steps,),
        in_specs=[pl.BlockSpec(memory_space=pltpu.SMEM), whole(x), whole(r), whole(dy), whole(gain), wcol(0), wcol(1), wcol(2),
                  pl.BlockSpec((hb, hidden), lambda j: (j, 0)), whole(cos), whole(sin)],
        out_specs=[full((1, hidden))] + [tok] * 8 + [pl.BlockSpec(back, lambda j: (0, 0, 0))] * n_dev,
        out_shape=[jax.ShapeDtypeStruct((1, hidden), F32)] + [jax.ShapeDtypeStruct((seq // 2, width), BF16)] * 8
        + [jax.ShapeDtypeStruct(back, BF16)] * n_dev,
        scratch_shapes=[pltpu.VMEM((seq, hidden), F32), pltpu.VMEM((seq, hidden), F32)],
        compiler_params=pltpu.CompilerParams(dimension_semantics=("arbitrary",), vmem_limit_bytes=60 << 20),
        cost_estimate=pl.CostEstimate(flops=60_000_000_000, bytes_accessed=60_000_000, transcendentals=8_000_000),
        name="block",
    )(me, x, r, dy, gain, w_qkv, w_qkv, w_qkv, w_out, cos, sin)


def join_kernel(me_ref, *refs):
    y_ref, dx_ref = refs[-2:]
    for m, ref in enumerate(refs[:-2]):
        owner = jnp.bitwise_xor(me_ref[0], m)
        y_ref[owner] = ref[0]
        dx_ref[owner] = ref[1]


def join_call(me, parts):
    n_dev = len(parts)
    _, piece, hidden = parts[0].shape
    return pl.pallas_call(
        join_kernel,
        in_specs=[pl.BlockSpec(memory_space=pltpu.SMEM)] + [pl.BlockSpec(memory_space=pltpu.VMEM)] * n_dev,
        out_shape=[jax.ShapeDtypeStruct((n_dev, piece, hidden), BF16)] * 2,
        compiler_params=pltpu.CompilerParams(vmem_limit_bytes=32 << 20),
        cost_estimate=pl.CostEstimate(flops=1_000_000, bytes_accessed=8_000_000, transcendentals=0),
        name="join",
    )(me, *parts)


def norm_kernel(both_ref, gain_ref, x_ref, dy_ref, r_ref, *pair_refs):
    n, rows, hidden = both_ref.shape
    piece = rows // 2
    xb = both_ref[:, :piece, :].reshape(n * piece, hidden)
    dy = both_ref[:, piece:, :].reshape(n * piece, hidden)
    x_ref[...] = xb
    dy_ref[...] = dy
    x = xb.astype(F32)
    inv = lax.rsqrt(jnp.mean(x * x, axis=1, keepdims=True) + NORM_EPS)
    r = (x * inv * gain_ref[...]).astype(BF16)
    r_ref[...] = r
    part = pair_refs[0].shape[2]
    for i, ref in enumerate(pair_refs):
        ref[0] = r[part * i:part * i + part].T
        ref[1] = dy[part * i:part * i + part].T


def norm_call(both, gain):
    n, rows, hidden = both.shape
    seq = n * rows // 2
    return pl.pallas_call(
        norm_kernel,
        out_shape=[jax.ShapeDtypeStruct((seq, hidden), BF16)] * 3 + [jax.ShapeDtypeStruct((2, hidden, seq // 2), BF16)] * 2,
        compiler_params=pltpu.CompilerParams(vmem_limit_bytes=48 << 20),
        cost_estimate=pl.CostEstimate(flops=10_000_000, bytes_accessed=14_000_000, transcendentals=0),
        name="norm",
    )(both, gain)


def grad_kernel(count, flip, add, *refs):
    lefts, rights = refs[:count], refs[count:2 * count]
    out_ref, l_buf, r_buf = refs[-3:]
    part = lefts[0].shape[2]

    @pl.when(pl.program_id(1) == 0)
    def _():
        for i, ref in enumerate(lefts):
            l_buf[:, part * i:part * i + part] = ref[0]

    for i, ref in enumerate(rights):
        r_buf[part * i:part * i + part, :] = ref[...]

    sub = 512

    def body(i, carry):
        rows = pl.ds(pl.multiple_of(i * sub, sub), sub)
        tile = dot(l_buf[rows, :], r_buf[...])
        if flip and add:
            out_ref[:, rows] = refs[2 * count][:, rows] + tile.T
        elif flip:
            out_ref[:, rows] = tile.T
        elif add:
            out_ref[rows, :] = refs[2 * count][rows, :] + tile
        else:
            out_ref[rows, :] = tile
        return carry

    lax.fori_loop(0, l_buf.shape[0] // sub, body, 0)


def grad_call(lefts, rights, which, n_out, col, buf=None, flip=False, add=False):
    count = len(lefts)
    _, rows, part = lefts[0].shape
    n = rights[0].shape[1]
    tm, tn = 1024, 512
    specs = [pl.BlockSpec((1, tm, part), lambda i, j: (which, i, 0))] * count + [pl.BlockSpec((part, tn), lambda i, j: (0, j))] * count
    args = list(lefts) + list(rights)
    if flip:
        out_spec = pl.BlockSpec((tn, tm), lambda i, j: (j, i))
        out_shape = jax.ShapeDtypeStruct((n, rows), F32)
    else:
        out_spec = pl.BlockSpec((tm, tn), lambda i, j: (i, col // tn + j))
        out_shape = jax.ShapeDtypeStruct((rows, n_out), F32)
    aliases = {}
    if buf is not None:
        specs.append(out_spec if add else pl.BlockSpec(memory_space=pl.ANY))
        args.append(buf)
        aliases = {2 * count: 0}
    return pl.pallas_call(
        functools.partial(grad_kernel, count, flip, add),
        grid=(rows // tm, n // tn),
        in_specs=specs,
        out_specs=out_spec,
        out_shape=out_shape,
        scratch_shapes=[pltpu.VMEM((tm, part * count), BF16), pltpu.VMEM((part * count, tn), BF16)],
        input_output_aliases=aliases,
        compiler_params=pltpu.CompilerParams(dimension_semantics=("arbitrary",) * 2, vmem_limit_bytes=56 << 20),
        cost_estimate=pl.CostEstimate(flops=2 * rows * n * part * count, bytes_accessed=80_000_000, transcendentals=0),
        name="wgrad",
    )(*args)


def solution(mesh):
    def device_fn(x_in, positions, long_factor, norm_gain, w_qkv, w_out, grad_y):
        _, _, hidden = x_in.shape
        n_dev = mesh.shape['cp']
        width = w_out.shape[0]
        scale = 1.0 / math.sqrt(2 * long_factor.shape[0])
        me = lax.axis_index('cp').astype(jnp.int32)[None]

        def shift(t, bit):
            return lax.ppermute(t, 'cp', [(i, i ^ bit) for i in range(n_dev)])

        def after(values, deps):
            return lax.optimization_barrier((values, deps))[0]

        both = lax.all_to_all(jnp.concatenate([x_in, grad_y], axis=1), 'cp', split_axis=0, concat_axis=0)
        pos = lax.all_gather(positions, 'cp', tiled=True)
        cos, sin = rope_tables(pos, long_factor)
        x, dy, r, pair_a, pair_b = norm_call(both, norm_gain[None, :])

        def own(ab):
            a, b = ab
            return [a, b, shift(a, 1), shift(b, 1)]

        def near(ab):
            a, b = ab
            return [shift(a, 2), shift(b, 2), shift(a, 4), shift(b, 4)]

        def far(part, deps=()):
            part = after(part, deps)
            diag = [shift(part[0], 4), shift(part[3], 2)]
            across = [shift(t, 1) for t in part]
            across += [shift(t, 1) for t in diag]
            return list(part) + diag + across

        p_ab = (pair_a, pair_b)
        p_part, p_own = near(p_ab), own(p_ab)
        out = block_call(me, x, r, dy, norm_gain[None, :], w_qkv, w_out, cos, sin, scale, n_dev)
        gg = out[0]
        o_ab, q_ab, k_ab, v_ab = (tuple(out[i:i + 2]) for i in (1, 3, 5, 7))
        back = out[9:]
        gg1 = shift(gg, 1)
        p_rest = far(p_part, (gg,))
        o_part = near(o_ab)
        cols = 3 * width
        g_wout = grad_call(p_own, own(o_ab), 1, hidden, 0, flip=True)
        g_wqkv = grad_call(p_own, own(q_ab), 0, cols, 0)
        g_wqkv = grad_call(p_own, own(k_ab), 0, cols, width, g_wqkv)
        g_wqkv = grad_call(p_own, own(v_ab), 0, cols, 2 * width, g_wqkv)
        gg, gg1 = after((gg, gg1), g_wqkv)
        gg = gg + gg1
        o_rest = far(o_part, (g_wqkv, g_wout))
        gg2 = shift(gg, 2)
        q_part = near(after(q_ab, o_part))
        back = list(back)
        early = (2, 4)
        for m in early:
            back[m] = shift(after(back[m], o_part), m)
        g_wout = grad_call(p_rest, o_rest, 1, hidden, 0, g_wout, flip=True, add=True)
        gg, gg2 = after((gg, gg2), g_wout)
        gg = gg + gg2
        q_rest = far(q_part, (g_wout,))
        gg4 = shift(gg, 4)
        k_part = near(after(k_ab, g_wout))
        v_part = near(after(v_ab, k_part))
        g_wqkv = grad_call(p_rest, q_rest, 0, cols, 0, g_wqkv, add=True)
        gg, gg4 = after((gg, gg4), g_wqkv)
        g_gain = (gg + gg4)[0]
        k_rest = far(k_part, (g_wqkv,))
        g_wqkv = grad_call(p_rest, k_rest, 0, cols, width, g_wqkv, add=True)
        v_rest = far(v_part, (g_wqkv,))
        for m in range(1, n_dev):
            if m not in early:
                back[m] = shift(after(back[m], g_wqkv), m)
        g_wqkv = grad_call(p_rest[:4], v_part, 0, cols, 2 * width, g_wqkv, add=True)
        g_wqkv = grad_call(p_rest[4:], v_rest[4:], 0, cols, 2 * width, g_wqkv, add=True)
        y_out, grad_x = join_call(*after((me, back), g_wqkv))
        return y_out, grad_x, g_gain, g_wqkv, g_wout

    seq_spec = P('dp', 'cp', None)
    return jax.shard_map(device_fn, mesh=mesh, in_specs=(seq_spec, P(('dp', 'cp')), P(None), P(None), P(None, None), P(None, None), seq_spec), out_specs=(seq_spec, seq_spec, P('dp'), P('dp', None), P('dp', None)), check_vma=False)
```
